32 devices in a mesh: row: 8 (over z, x), col: 4 (over y, core).
Axes of the slice: x: 2, y: 2, z: 4, core: 2. Of those that a mesh axis runs over, the one named last changes fastest.
Arguments:
- rhs: bfloat16 [2, 4096, 2048], P(None, 'row', 'col'), may hold values from -6 to 6
- panel: bfloat16 [2, 4096, 1024], P(None, 'row', 'col'), may hold values from -0.25 to 0.25
- pivots: float32 [1024], P('col'), may hold values from 2 to 4
Outputs:
- updated: float32 [2, 4096, 2048], P(None, 'row', 'col')
The draws below stay inside these ranges and needn't reach their ends.
All inputs are finite; a program needn't handle non-finite values.
Results may differ from the reference program's by a relative error of at most 0.0045.
Values may be sent and summed in bfloat16 or wider, within the bound.
A program may use at most 64 MiB of HBM per device.

```python
import math
import jax
import jax.numpy as jnp
from jax import lax

BLK = 512
T_DEV = 2
COLS_DEV = 512
ROWS = 4096
COLS = 2048


def steps_of(stream_key, dims, cuts, least, largest):
    loudness = 1.0
    for axis_at, blocks in cuts:
        draws = jax.random.uniform(jax.random.fold_in(jax.random.fold_in(stream_key, 6), axis_at), (blocks,), jnp.float32, least / len(cuts), largest / len(cuts))
        loudness = loudness * jnp.repeat(jnp.exp(draws), dims[axis_at] // blocks).reshape((-1,) + (1,) * (len(dims) - 1 - axis_at))
    return loudness


def scatter_about(key, shape, scale, limit, cuts=(), held_as=jnp.bfloat16):
    entries = scale * jax.random.normal(key, shape, jnp.float32)
    if cuts:
        entries = entries * steps_of(key, shape, cuts, -0.22, 0.18)
    return jnp.clip(entries, -limit, limit).astype(held_as)


def setup_inputs(seed: int = 0) -> dict:
    seeds = jax.random.split(jax.random.key(seed), 4)
    rhs = scatter_about(seeds[0], (T_DEV, ROWS, COLS), 1.0, 6.0, ((1, 8), (2, 4)))
    panel = scatter_about(seeds[1], (T_DEV, ROWS, 2 * BLK), BLK ** -0.5, 0.25, ((1, 8), (2, 4)))
    pivots = jnp.clip(jnp.exp(math.log(4.0) - 0.6931472 * jax.random.uniform(seeds[2], (2 * BLK,), jnp.float32) ** steps_of(seeds[2], (2 * BLK,), ((0, 4),), -0.2, 0.2)), 2.0, 4.0)
    return dict(rhs=rhs, panel=panel, pivots=pivots)


def lower_solve(matrix, values):
    return lax.linalg.triangular_solve(matrix, values, left_side=True, lower=True)

def reference(rhs, panel, pivots):
    layers = rhs.shape[0]
    rows = rhs.shape[1]
    cols = rhs.shape[2]
    left = panel.reshape(layers * rows, 2 * BLK)
    lower_zero = jnp.tril(panel[0, 0:BLK, 0:BLK].astype(jnp.float32), -1) + jnp.diag(pivots[0:BLK])
    lower_one = jnp.tril(panel[0, BLK:2 * BLK, BLK:2 * BLK].astype(jnp.float32), -1) + jnp.diag(pivots[BLK:2 * BLK])
    width = COLS_DEV
    blocks = cols // width
    stacked = rhs.reshape(layers * rows, blocks, width).transpose(1, 0, 2)

    def solve_block(block):
        values = block.astype(jnp.float32)
        first = lower_solve(lower_zero, values[0:BLK])
        first_low = first.astype(jnp.bfloat16)
        values = values - jnp.dot(left[:, 0:BLK].astype(jnp.float32), first_low.astype(jnp.float32), preferred_element_type=jnp.float32)
        second = lower_solve(lower_one, values[BLK:2 * BLK])
        second_low = second.astype(jnp.bfloat16)
        values = values - jnp.dot(left[:, BLK:2 * BLK].astype(jnp.float32), second_low.astype(jnp.float32), preferred_element_type=jnp.float32)
        values = values.at[0:BLK].set(first)
        values = values.at[BLK:2 * BLK].set(second)
        return values
    solved = lax.map(solve_block, stacked)
    return solved.transpose(1, 0, 2).reshape(layers, rows, cols)
```

```python
import functools

import jax
import jax.numpy as jnp
from jax import lax
from jax.experimental import pallas as pl
from jax.experimental.pallas import tpu as pltpu
from jax.sharding import PartitionSpec as P

MESH = pl.DeviceIdType.MESH
LANES = 128
PIECES = 2
HALVES = 2
F32 = jnp.float32
BF16 = jnp.bfloat16


def mm(a, b):
    return jnp.dot(a, b, preferred_element_type=F32)


def mm32(a, b):
    return jnp.dot(a, b, preferred_element_type=F32, precision=lax.Precision.HIGHEST)


def split(a):
    high = a.astype(BF16)
    return high, (a - high.astype(F32)).astype(BF16)


def unit_inverse(n):
    size = n.shape[0]
    if size > LANES:
        half = size // 2
        top = unit_inverse(n[:half, :half])
        low = unit_inverse(n[half:, half:])
        corner = -mm32(low, mm32(n[half:, :half], top))
        return jnp.concatenate(
            [
                jnp.concatenate([top, jnp.zeros((half, half), F32)], axis=1),
                jnp.concatenate([corner, low], axis=1),
            ],
            axis=0,
        )
    row = lax.broadcasted_iota(jnp.int32, (size, size), 0)
    col = lax.broadcasted_iota(jnp.int32, (size, size), 1)
    base = 4
    small = jnp.where((row >> base) == (col >> base), n, 0.0)
    total = jnp.where(row == col, 1.0, 0.0) - small
    power = small
    for _ in range(base - 1):
        power = mm32(power, power)
        total = total + mm32(total, power)
    shift = base
    while (1 << shift) < size:
        inside = ((row >> (shift + 1)) == (col >> (shift + 1))) & (
            (row >> shift) != (col >> shift)
        )
        total = total - mm32(total, mm32(jnp.where(inside, n, 0.0), total))
        shift += 1
    return total


def kernel(
    rows,
    cols,
    rhs,
    panel,
    pivots,
    out,
    gat,
    piv,
    xl,
    low_tri,
    inv_hi,
    inv_lo,
    scale,
    g_send,
    g_recv,
    f_send,
    p_send,
    p_recv,
    z_send,
    x_send,
    x_recv,
):
    r = lax.axis_index("row")
    c = lax.axis_index("col")
    line = lax.rem(r, 2)
    depth = r // 2
    depths = rows // 2
    layers, width, columns = rhs.shape
    cw = panel.shape[2]
    half = cols // 2
    ys = cols // 2
    y, core = c // 2, lax.rem(c, 2)
    chunks = columns // LANES
    piece_rows = width // PIECES
    part_rows = width // HALVES
    partner = y * 2 + 1 - core

    barrier = pltpu.get_barrier_semaphore()
    for d in range(1, cols):
        pl.semaphore_signal(
            barrier, inc=1, device_id={"col": lax.rem(c + d, cols)}, device_id_type=MESH
        )
    pl.semaphore_signal(
        barrier, inc=1, device_id={"row": depth * 2 + 1 - line}, device_id_type=MESH
    )

    @pl.when(depth > 0)
    def _():
        pl.semaphore_signal(barrier, inc=1, device_id={"row": r - 2}, device_id_type=MESH)

    @pl.when(depth < depths - 1)
    def _():
        pl.semaphore_signal(barrier, inc=1, device_id={"row": r + 2}, device_id_type=MESH)

    peers = cols + jnp.where(depth > 0, 1, 0) + jnp.where(depth < depths - 1, 1, 0)
    pl.semaphore_wait(barrier, peers)

    def own(k, t, h):
        part = pl.ds(h * part_rows, part_rows)
        target = partner if k == 0 else lax.rem(y + k, ys) * 2 + core
        return pltpu.make_async_remote_copy(
            src_ref=panel.at[t, part],
            dst_ref=gat.at[c, t, part],
            send_sem=g_send.at[k, t, h],
            recv_sem=g_recv.at[c, t, h],
            device_id={"col": target},
            device_id_type=MESH,
        )

    def relay(k, t, h):
        part = pl.ds(h * part_rows, part_rows)
        source = lax.rem(y + ys - k, ys) * 2 + core
        return pltpu.make_async_remote_copy(
            src_ref=gat.at[source, t, part],
            dst_ref=gat.at[source, t, part],
            send_sem=f_send.at[k, t, h],
            recv_sem=g_recv.at[source, t, h],
            device_id={"col": partner},
            device_id_type=MESH,
        )

    def arrived(source, t, h):
        part = pl.ds(h * part_rows, part_rows)
        pltpu.make_async_remote_copy(
            src_ref=gat.at[source, t, part],
            dst_ref=gat.at[source, t, part],
            send_sem=f_send.at[0, t, h],
            recv_sem=g_recv.at[source, t, h],
            device_id={"col": partner},
            device_id_type=MESH,
        ).wait_recv()

    def pivot_copy(d, source):
        return pltpu.make_async_remote_copy(
            src_ref=pivots,
            dst_ref=piv.at[source],
            send_sem=p_send.at[d],
            recv_sem=p_recv.at[source],
            device_id={"col": lax.rem(c + d, cols)},
            device_id_type=MESH,
        )

    @pl.when(depth == 0)
    def _():
        for d in range(1, cols):
            pivot_copy(d, c).start()

    for t in range(layers):
        for h in range(HALVES):
            for k in range(ys):
                own(k, t, h).start()
    gat[c] = panel[...]

    def take_layer(t):
        for h in range(HALVES):
            for k in range(1, ys):
                source = lax.rem(y + ys - k, ys) * 2 + core
                arrived(source, t, h)
                relay(k, t, h).start()
        for h in range(HALVES):
            for k in range(ys):
                arrived(lax.rem(y + ys - k, ys) * 2 + 1 - core, t, h)

    take_layer(0)

    def piece(s, n, q):
        return xl.at[s, n, pl.ds(q * piece_rows, piece_rows)]

    def down(s, n, q):
        return pltpu.make_async_remote_copy(
            src_ref=piece(s, n, q),
            dst_ref=piece(s, n, q),
            send_sem=z_send.at[n, q],
            recv_sem=x_recv.at[s, n, q],
            device_id={"row": r + 2},
            device_id_type=MESH,
        )

    def across(s, n, q):
        return pltpu.make_async_remote_copy(
            src_ref=piece(s, n, q),
            dst_ref=piece(s, n, q),
            send_sem=x_send.at[n, q],
            recv_sem=x_recv.at[s, n, q],
            device_id={"row": depth * 2 + 1 - line},
            device_id_type=MESH,
        )

    def forward(n, q):
        across(line, n, q).start()

        @pl.when(depth < depths - 1)
        def _():
            down(line, n, q).start()

    def lanes(n):
        return pl.ds(pl.multiple_of(n * LANES, LANES), LANES)

    def product(s, t, n):
        total = None
        for j in range(half):
            term = mm(gat[s * half + j, t], xl[s, n, pl.ds(j * cw, cw)])
            total = term if total is None else total + term
        return total

    @pl.when(depth == 0)
    def _():
        for d in range(1, cols):
            pivot_copy(d, lax.rem(c + d, cols)).wait_recv()
        piv[c] = pivots[...]
        for j in range(half):
            low_tri[:, j * cw : (j + 1) * cw] = gat[line * half + j, 0]
        recip = 1.0 / jnp.concatenate([piv[line * half + j] for j in range(half)], axis=1)
        row = lax.broadcasted_iota(jnp.int32, (width, width), 0)
        col = lax.broadcasted_iota(jnp.int32, (width, width), 1)
        scaled = jnp.where(row > col, low_tri[...].astype(F32) * recip, 0.0)
        scale[...] = jnp.broadcast_to(
            jnp.sum(jnp.where(row == col, recip, 0.0), axis=1, keepdims=True), scale.shape
        )
        high, low = split(unit_inverse(scaled))
        inv_hi[...] = high
        inv_lo[...] = low

    @pl.when(r == 0)
    def _():
        @pl.loop(0, chunks)
        def _(n):
            side = rhs[0, :, lanes(n)]
            x = (mm(inv_hi[...], side) + mm(inv_lo[...], side)) * scale[...]
            xl[0, n] = x.astype(BF16)
            out[0, :, lanes(n)] = x
            for q in range(PIECES):
                forward(n, q)

    @pl.when(r == 1)
    def _():
        @pl.loop(0, chunks)
        def _(n):
            for q in range(PIECES):
                across(0, n, q).wait_recv()
            side = rhs[0, :, lanes(n)].astype(F32) - product(0, 0, n)
            high, low = split(side)
            x = (mm(inv_hi[...], high) + mm(inv_lo[...], high) + mm(inv_hi[...], low)) * scale[...]
            xl[1, n] = x.astype(BF16)
            out[0, :, lanes(n)] = x
            for q in range(PIECES):
                forward(n, q)

    for t in range(1, layers):
        take_layer(t)

    @pl.loop(0, chunks)
    def _(n):
        @pl.when(depth > 0)
        def _():
            for q in range(PIECES):
                across(line, n, q).wait_recv()
                forward(n, q)
            out[0, :, lanes(n)] = rhs[0, :, lanes(n)].astype(F32) - product(line, 0, n)

        for t in range(1, layers):
            out[t, :, lanes(n)] = rhs[t, :, lanes(n)].astype(F32) - product(line, t, n)

    other = 1 - line

    @pl.loop(0, chunks)
    def _(n):
        @pl.when(r != 1)
        def _():
            for q in range(PIECES):
                across(other, n, q).wait_recv()

        @pl.when(depth > 0)
        def _():
            out[0, :, lanes(n)] -= product(other, 0, n)

        for t in range(1, layers):
            out[t, :, lanes(n)] -= product(other, t, n)

    for t in range(layers):
        for h in range(HALVES):
            for k in range(ys):
                own(k, t, h).wait_send()
            for k in range(1, ys):
                relay(k, t, h).wait_send()

    @pl.when(depth == 0)
    def _():
        for d in range(1, cols):
            pivot_copy(d, c).wait_send()

    @pl.loop(0, chunks)
    def _(n):
        for q in range(PIECES):
            across(line, n, q).wait_send()

            @pl.when(depth < depths - 1)
            def _():
                down(line, n, q).wait_send()


def on_device(rows, cols, rhs, panel, pivots):
    layers, width, columns = rhs.shape
    cw = panel.shape[2]
    pw = pivots.shape[0]
    ys = cols // 2
    chunks = columns // LANES
    dma = pltpu.SemaphoreType.DMA
    vmem = pl.BlockSpec(memory_space=pltpu.VMEM)
    return pl.pallas_call(
        functools.partial(kernel, rows, cols),
        out_shape=jax.ShapeDtypeStruct((layers, width, columns), F32),
        in_specs=[vmem] * 3,
        out_specs=vmem,
        scratch_shapes=[
            pltpu.VMEM((cols, layers, width, cw), BF16),
            pltpu.VMEM((cols, 1, pw), F32),
            pltpu.VMEM((2, chunks, width, LANES), BF16),
            pltpu.VMEM((width, width), BF16),
            pltpu.VMEM((width, width), BF16),
            pltpu.VMEM((width, width), BF16),
            pltpu.VMEM((width, LANES), F32),
            dma((ys, layers, HALVES)),
            dma((cols, layers, HALVES)),
            dma((ys, layers, HALVES)),
            dma((cols,)),
            dma((cols,)),
            dma((chunks, PIECES)),
            dma((chunks, PIECES)),
            dma((2, chunks, PIECES)),
        ],
        compiler_params=pltpu.CompilerParams(
            collective_id=0, has_side_effects=True, vmem_limit_bytes=56 * 1024 * 1024
        ),
        name="solve_and_update",
    )(rhs, panel, pivots.reshape(1, pw))


def solution(mesh):
    placed = (P(None, "row", "col"), P(None, "row", "col"), P("col"))
    return jax.shard_map(
        functools.partial(on_device, mesh.shape["row"], mesh.shape["col"]),
        mesh=mesh,
        in_specs=placed,
        out_specs=P(None, "row", "col"),
        check_vma=False,
    )
```

```python
import functools

import jax
import jax.numpy as jnp
from jax import lax
from jax.experimental import pallas as pl
from jax.experimental.pallas import tpu as pltpu
from jax.sharding import PartitionSpec as P

MESH = pl.DeviceIdType.MESH
LANES = 128
PIECES = 2
HALVES = 2
F32 = jnp.float32
BF16 = jnp.bfloat16


def mm(a, b):
    return jnp.dot(a, b, preferred_element_type=F32)


def split(a):
    high = a.astype(BF16)
    return high, (a - high.astype(F32)).astype(BF16)


def mm3(a, b):
    ah, al = split(a)
    bh, bl = split(b)
    return mm(ah, bh) + (mm(ah, bl) + mm(al, bh))


def unit_inverse(n):
    width = n.shape[0]
    row = lax.broadcasted_iota(jnp.int32, (LANES, LANES), 0)
    col = lax.broadcasted_iota(jnp.int32, (LANES, LANES), 1)
    base = 4
    blocks = [n[i : i + LANES, i : i + LANES] for i in range(0, width, LANES)]
    power = [jnp.where((row >> base) == (col >> base), b, 0.0) for b in blocks]
    done = [jnp.where(row == col, 1.0, 0.0) - p for p in power]
    for _ in range(base - 1):
        power = [mm3(p, p) for p in power]
        done = [d + mm3(d, p) for d, p in zip(done, power)]
    shift = base
    while (1 << shift) < LANES:
        inside = ((row >> (shift + 1)) == (col >> (shift + 1))) & (
            (row >> shift) != (col >> shift)
        )
        right = [mm3(jnp.where(inside, b, 0.0), d) for b, d in zip(blocks, done)]
        done = [d - mm3(d, m) for d, m in zip(done, right)]
        shift += 1
    size = LANES
    while size < width:
        pairs = []
        for i in range(0, len(done), 2):
            top, low, at = done[i], done[i + 1], i * size
            corner = -mm3(low, mm3(n[at + size : at + 2 * size, at : at + size], top))
            first = jnp.concatenate([top, jnp.zeros((size, size), F32)], axis=1)
            pairs.append(
                jnp.concatenate([first, jnp.concatenate([corner, low], axis=1)], axis=0)
            )
        done = pairs
        size *= 2
    return done[0]


def kernel(
    rows,
    cols,
    rhs_in,
    panel_in,
    pivots,
    out_to,
    rhs,
    out,
    gat,
    piv,
    xl,
    low_tri,
    inv_hi,
    inv_lo,
    scale,
    g_send,
    g_recv,
    f_send,
    p_send,
    p_recv,
    z_send,
    x_send,
    x_recv,
    in_sem,
    out_sem,
):
    r = lax.axis_index("row")
    c = lax.axis_index("col")
    line = lax.rem(r, 2)
    depth = r // 2
    depths = rows // 2
    layers, width, columns = rhs.shape
    cw = panel_in.shape[2]
    half = cols // 2
    ys = cols // 2
    y, core = c // 2, lax.rem(c, 2)
    chunks = columns // LANES
    piece_rows = width // PIECES
    part_rows = width // HALVES
    partner = y * 2 + 1 - core

    panel_copy = pltpu.make_async_copy(panel_in, gat.at[c], in_sem.at[0])
    rhs_copy = pltpu.make_async_copy(rhs_in, rhs, in_sem.at[1])
    panel_copy.start()
    rhs_copy.start()

    barrier = pltpu.get_barrier_semaphore()
    for d in range(1, cols):
        pl.semaphore_signal(
            barrier, inc=1, device_id={"col": lax.rem(c + d, cols)}, device_id_type=MESH
        )
    pl.semaphore_signal(
        barrier, inc=1, device_id={"row": depth * 2 + 1 - line}, device_id_type=MESH
    )

    @pl.when(depth > 0)
    def _():
        pl.semaphore_signal(barrier, inc=1, device_id={"row": r - 2}, device_id_type=MESH)

    @pl.when(depth < depths - 1)
    def _():
        pl.semaphore_signal(barrier, inc=1, device_id={"row": r + 2}, device_id_type=MESH)

    peers = cols + jnp.where(depth > 0, 1, 0) + jnp.where(depth < depths - 1, 1, 0)
    pl.semaphore_wait(barrier, peers)

    def own(k, t, h):
        part = pl.ds(h * part_rows, part_rows)
        target = partner if k == 0 else lax.rem(y + k, ys) * 2 + core
        return pltpu.make_async_remote_copy(
            src_ref=gat.at[c, t, part],
            dst_ref=gat.at[c, t, part],
            send_sem=g_send.at[k, t, h],
            recv_sem=g_recv.at[c, t, h],
            device_id={"col": target},
            device_id_type=MESH,
        )

    def relay(k, t, h):
        part = pl.ds(h * part_rows, part_rows)
        source = lax.rem(y + ys - k, ys) * 2 + core
        return pltpu.make_async_remote_copy(
            src_ref=gat.at[source, t, part],
            dst_ref=gat.at[source, t, part],
            send_sem=f_send.at[k, t, h],
            recv_sem=g_recv.at[source, t, h],
            device_id={"col": partner},
            device_id_type=MESH,
        )

    def arrived(source, t, h):
        part = pl.ds(h * part_rows, part_rows)
        pltpu.make_async_remote_copy(
            src_ref=gat.at[source, t, part],
            dst_ref=gat.at[source, t, part],
            send_sem=f_send.at[0, t, h],
            recv_sem=g_recv.at[source, t, h],
            device_id={"col": partner},
            device_id_type=MESH,
        ).wait_recv()

    def pivot_copy(d, source):
        return pltpu.make_async_remote_copy(
            src_ref=pivots,
            dst_ref=piv.at[source],
            send_sem=p_send.at[d],
            recv_sem=p_recv.at[source],
            device_id={"col": lax.rem(c + d, cols)},
            device_id_type=MESH,
        )

    @pl.when(depth == 0)
    def _():
        for d in range(1, cols):
            pivot_copy(d, c).start()

    def needed(source, t, h, do):
        if t > 0:
            do()
            return
        read = (source < half) & ((h + 1) * part_rows > source * cw)

        @pl.when((r > 0) | read)
        def _():
            do()

    panel_copy.wait()
    for t in range(layers):
        for h in range(HALVES):
            for k in range(ys - 1, -1, -1):
                needed(c, t, h, lambda: own(k, t, h).start())

    def take_layer(t):
        for h in range(HALVES):
            for k in range(1, ys):
                source = lax.rem(y + ys - k, ys) * 2 + core

                def pass_on():
                    arrived(source, t, h)
                    relay(k, t, h).start()

                needed(source, t, h, pass_on)
        for h in range(HALVES):
            for k in range(ys):
                source = lax.rem(y + ys - k, ys) * 2 + 1 - core
                needed(source, t, h, lambda: arrived(source, t, h))

    take_layer(0)

    def piece(s, n, q):
        return xl.at[s, n, pl.ds(q * piece_rows, piece_rows)]

    def down(s, n, q):
        return pltpu.make_async_remote_copy(
            src_ref=piece(s, n, q),
            dst_ref=piece(s, n, q),
            send_sem=z_send.at[n, q],
            recv_sem=x_recv.at[s, n, q],
            device_id={"row": r + 2},
            device_id_type=MESH,
        )

    def across(s, n, q):
        return pltpu.make_async_remote_copy(
            src_ref=piece(s, n, q),
            dst_ref=piece(s, n, q),
            send_sem=x_send.at[n, q],
            recv_sem=x_recv.at[s, n, q],
            device_id={"row": depth * 2 + 1 - line},
            device_id_type=MESH,
        )

    def forward(n, q):
        across(line, n, q).start()

        @pl.when(depth < depths - 1)
        def _():
            down(line, n, q).start()

    def lanes(n):
        return pl.ds(pl.multiple_of(n * LANES, LANES), LANES)

    def product(s, t, n):
        total = None
        for j in range(half):
            term = mm(gat[s * half + j, t], xl[s, n, pl.ds(j * cw, cw)])
            total = term if total is None else total + term
        return total

    @pl.when(depth == 0)
    def _():
        for d in range(1, cols):
            pivot_copy(d, lax.rem(c + d, cols)).wait_recv()
        piv[c] = pivots[...]
        for j in range(half):
            low_tri[:, j * cw : (j + 1) * cw] = gat[line * half + j, 0]
        recip = 1.0 / jnp.concatenate([piv[line * half + j] for j in range(half)], axis=1)
        row = lax.broadcasted_iota(jnp.int32, (width, width), 0)
        col = lax.broadcasted_iota(jnp.int32, (width, width), 1)
        scaled = jnp.where(row > col, low_tri[...].astype(F32) * recip, 0.0)
        scale[...] = jnp.broadcast_to(
            jnp.sum(jnp.where(row == col, recip, 0.0), axis=1, keepdims=True), scale.shape
        )
        high, low = split(unit_inverse(scaled))
        inv_hi[...] = high
        inv_lo[...] = low

    rhs_copy.wait()

    @pl.when(r == 0)
    def _():
        @pl.loop(0, chunks)
        def _(n):
            side = rhs[0, :, lanes(n)]
            x = (mm(inv_hi[...], side) + mm(inv_lo[...], side)) * scale[...]
            xl[0, n] = x.astype(BF16)
            out[0, :, lanes(n)] = x
            for q in range(PIECES):
                forward(n, q)

    @pl.when(r == 1)
    def _():
        @pl.loop(0, chunks)
        def _(n):
            for q in range(PIECES):
                across(0, n, q).wait_recv()
            side = rhs[0, :, lanes(n)].astype(F32) - product(0, 0, n)
            high, low = split(side)
            x = (mm(inv_hi[...], high) + mm(inv_lo[...], high) + mm(inv_hi[...], low)) * scale[...]
            xl[1, n] = x.astype(BF16)
            out[0, :, lanes(n)] = x
            for q in range(PIECES):
                forward(n, q)

    for t in range(1, layers):
        take_layer(t)

    def leave(n):
        return pltpu.make_async_copy(
            out.at[:, :, lanes(n)], out_to.at[:, :, lanes(n)], out_sem.at[n]
        )

    def start(t, n):
        return rhs[t, :, lanes(n)].astype(F32)

    @pl.when(line == 0)
    def _():
        @pl.loop(0, chunks)
        def _(n):
            @pl.when(depth > 0)
            def _():
                for q in range(PIECES):
                    across(0, n, q).wait_recv()
                    forward(n, q)
                out[0, :, lanes(n)] = start(0, n) - product(0, 0, n)

            for t in range(1, layers):
                out[t, :, lanes(n)] = start(t, n) - product(0, t, n)

        @pl.loop(0, chunks)
        def _(n):
            for q in range(PIECES):
                across(1, n, q).wait_recv()

            @pl.when(depth > 0)
            def _():
                out[0, :, lanes(n)] -= product(1, 0, n)

            for t in range(1, layers):
                out[t, :, lanes(n)] -= product(1, t, n)
            leave(n).start()

    @pl.when(line == 1)
    def _():
        @pl.loop(0, chunks)
        def _(n):
            @pl.when(depth > 0)
            def _():
                for q in range(PIECES):
                    across(1, n, q).wait_recv()
                    forward(n, q)
                for q in range(PIECES):
                    across(0, n, q).wait_recv()
                out[0, :, lanes(n)] = start(0, n) - product(0, 0, n) - product(1, 0, n)

            for t in range(1, layers):
                out[t, :, lanes(n)] = start(t, n) - product(0, t, n) - product(1, t, n)
            leave(n).start()

    for t in range(layers):
        for h in range(HALVES):
            for k in range(ys):
                needed(c, t, h, lambda: own(k, t, h).wait_send())
            for k in range(1, ys):
                source = lax.rem(y + ys - k, ys) * 2 + core
                needed(source, t, h, lambda: relay(k, t, h).wait_send())

    @pl.when(depth == 0)
    def _():
        for d in range(1, cols):
            pivot_copy(d, c).wait_send()

    @pl.loop(0, chunks)
    def _(n):
        for q in range(PIECES):
            across(line, n, q).wait_send()

            @pl.when(depth < depths - 1)
            def _():
                down(line, n, q).wait_send()

        leave(n).wait()


def on_device(rows, cols, rhs, panel, pivots):
    layers, width, columns = rhs.shape
    cw = panel.shape[2]
    pw = pivots.shape[0]
    ys = cols // 2
    chunks = columns // LANES
    dma = pltpu.SemaphoreType.DMA
    vmem = pl.BlockSpec(memory_space=pltpu.VMEM)
    anywhere = pl.BlockSpec(memory_space=pl.ANY)
    far = pl.BlockSpec(memory_space=pltpu.HBM)
    return pl.pallas_call(
        functools.partial(kernel, rows, cols),
        out_shape=jax.ShapeDtypeStruct((layers, width, columns), F32),
        in_specs=[far, far, vmem],
        out_specs=anywhere,
        scratch_shapes=[
            pltpu.VMEM((layers, width, columns), BF16),
            pltpu.VMEM((layers, width, columns), F32),
            pltpu.VMEM((cols, layers, width, cw), BF16),
            pltpu.VMEM((cols, 1, pw), F32),
            pltpu.VMEM((2, chunks, width, LANES), BF16),
            pltpu.VMEM((width, width), BF16),
            pltpu.VMEM((width, width), BF16),
            pltpu.VMEM((width, width), BF16),
            pltpu.VMEM((width, LANES), F32),
            dma((ys, layers, HALVES)),
            dma((cols, layers, HALVES)),
            dma((ys, layers, HALVES)),
            dma((cols,)),
            dma((cols,)),
            dma((chunks, PIECES)),
            dma((chunks, PIECES)),
            dma((2, chunks, PIECES)),
            dma((2,)),
            dma((chunks,)),
        ],
        compiler_params=pltpu.CompilerParams(
            collective_id=0, has_side_effects=True, vmem_limit_bytes=24 * 1024 * 1024
        ),
        name="solve_and_update",
    )(rhs, panel, pivots.reshape(1, pw))


def solution(mesh):
    placed = (P(None, "row", "col"), P(None, "row", "col"), P("col"))
    return jax.shard_map(
        functools.partial(on_device, mesh.shape["row"], mesh.shape["col"]),
        mesh=mesh,
        in_specs=placed,
        out_specs=P(None, "row", "col"),
        check_vma=False,
    )
```

```python
import functools

import jax
import jax.numpy as jnp
from jax import lax
from jax.experimental import pallas as pl
from jax.experimental.pallas import tpu as pltpu
from jax.sharding import PartitionSpec as P

MESH = pl.DeviceIdType.MESH
LANES = 128
PIECES = 4
HALVES = 4
F32 = jnp.float32
BF16 = jnp.bfloat16


def mm(a, b):
    return jnp.dot(a, b, preferred_element_type=F32)


def split(a):
    high = a.astype(BF16)
    return high, (a - high.astype(F32)).astype(BF16)


def mm3(a, b):
    ah, al = split(a)
    bh, bl = split(b)
    return mm(ah, bh) + (mm(ah, bl) + mm(al, bh))


def unit_inverses(parts):
    size, whole = LANES, parts[0].shape[0]
    row = lax.broadcasted_iota(jnp.int32, (LANES, LANES), 0)
    col = lax.broadcasted_iota(jnp.int32, (LANES, LANES), 1)
    base = 4
    blocks = [n[i : i + LANES, i : i + LANES] for n in parts for i in range(0, whole, LANES)]
    power = [jnp.where((row >> base) == (col >> base), b, 0.0) for b in blocks]
    done = [jnp.where(row == col, 1.0, 0.0) - p for p in power]
    for _ in range(base - 1):
        power = [mm3(p, p) for p in power]
        done = [d + mm3(d, p) for d, p in zip(done, power)]
    shift = base
    while (1 << shift) < LANES:
        inside = ((row >> (shift + 1)) == (col >> (shift + 1))) & (
            (row >> shift) != (col >> shift)
        )
        right = [mm3(jnp.where(inside, b, 0.0), d) for b, d in zip(blocks, done)]
        done = [d - mm3(d, m) for d, m in zip(done, right)]
        shift += 1
    while size < whole:
        each = whole // (2 * size)
        pairs = []
        for i in range(0, len(done), 2):
            n, at = parts[i // 2 // each], (i // 2 % each) * 2 * size
            top, low = done[i], done[i + 1]
            corner = -mm3(low, mm3(n[at + size : at + 2 * size, at : at + size], top))
            first = jnp.concatenate([top, jnp.zeros((size, size), F32)], axis=1)
            pairs.append(
                jnp.concatenate([first, jnp.concatenate([corner, low], axis=1)], axis=0)
            )
        done = pairs
        size *= 2
    return done


def kernel(
    rows,
    cols,
    rhs_in,
    panel_in,
    pivots,
    out_to,
    rhs,
    out,
    gat,
    piv,
    xl,
    low_tri,
    inv_hi,
    inv_lo,
    scale,
    ends,
    g_send,
    g_recv,
    f_send,
    p_send,
    p_recv,
    z_send,
    x_send,
    x_recv,
    in_sem,
    out_sem,
):
    r = lax.axis_index("row")
    c = lax.axis_index("col")
    line = lax.rem(r, 2)
    depth = r // 2
    depths = rows // 2
    layers, width, columns = rhs.shape
    cw = panel_in.shape[2]
    half = cols // 2
    ys = cols // 2
    y, core = c // 2, lax.rem(c, 2)
    chunks = columns // LANES
    piece_rows = width // PIECES
    part_rows = width // HALVES
    partner = y * 2 + 1 - core

    panel_copy = pltpu.make_async_copy(panel_in, gat.at[c], in_sem.at[0])
    rhs_copy = pltpu.make_async_copy(rhs_in, rhs, in_sem.at[1])
    panel_copy.start()
    rhs_copy.start()

    barrier = pltpu.get_barrier_semaphore()
    for d in range(1, cols):
        pl.semaphore_signal(
            barrier, inc=1, device_id={"col": lax.rem(c + d, cols)}, device_id_type=MESH
        )
    pl.semaphore_signal(
        barrier, inc=1, device_id={"row": depth * 2 + 1 - line}, device_id_type=MESH
    )

    @pl.when(depth > 0)
    def _():
        pl.semaphore_signal(barrier, inc=1, device_id={"row": r - 2}, device_id_type=MESH)

    @pl.when(depth < depths - 1)
    def _():
        pl.semaphore_signal(barrier, inc=1, device_id={"row": r + 2}, device_id_type=MESH)

    peers = cols + jnp.where(depth > 0, 1, 0) + jnp.where(depth < depths - 1, 1, 0)
    pl.semaphore_wait(barrier, peers)

    def own(k, t, h):
        part = pl.ds(h * part_rows, part_rows)
        target = partner if k == 0 else lax.rem(y + k, ys) * 2 + core
        return pltpu.make_async_remote_copy(
            src_ref=gat.at[c, t, part],
            dst_ref=gat.at[c, t, part],
            send_sem=g_send.at[k, t, h],
            recv_sem=g_recv.at[c, t, h],
            device_id={"col": target},
            device_id_type=MESH,
        )

    def relay(k, t, h):
        part = pl.ds(h * part_rows, part_rows)
        source = lax.rem(y + ys - k, ys) * 2 + core
        return pltpu.make_async_remote_copy(
            src_ref=gat.at[source, t, part],
            dst_ref=gat.at[source, t, part],
            send_sem=f_send.at[k, t, h],
            recv_sem=g_recv.at[source, t, h],
            device_id={"col": partner},
            device_id_type=MESH,
        )

    def arrived(source, t, h):
        part = pl.ds(h * part_rows, part_rows)
        pltpu.make_async_remote_copy(
            src_ref=gat.at[source, t, part],
            dst_ref=gat.at[source, t, part],
            send_sem=f_send.at[0, t, h],
            recv_sem=g_recv.at[source, t, h],
            device_id={"col": partner},
            device_id_type=MESH,
        ).wait_recv()

    def pivot_copy(d, source):
        return pltpu.make_async_remote_copy(
            src_ref=pivots,
            dst_ref=piv.at[source],
            send_sem=p_send.at[d],
            recv_sem=p_recv.at[source],
            device_id={"col": lax.rem(c + d, cols)},
            device_id_type=MESH,
        )

    @pl.when(depth == 0)
    def _():
        for d in range(1, cols):
            pivot_copy(d, c).start()

    def below(source, h):
        return h // (HALVES // 2) - source // (half // 2)

    def when_needed(source, t, h, do):
        if t > 0:
            do()
        else:
            pl.when((r > 0) | (below(source, h) >= 0))(do)

    panel_copy.wait()
    for t in range(layers):
        for h in range(HALVES):
            for k in range(ys - 1, -1, -1):
                when_needed(c, t, h, lambda: own(k, t, h).start())

    def take(t, wanted):
        for h in range(HALVES):
            for k in range(1, ys):
                source = lax.rem(y + ys - k, ys) * 2 + core

                def pass_on():
                    arrived(source, t, h)
                    relay(k, t, h).start()

                wanted(source, h, pass_on)
        for h in range(HALVES):
            for k in range(ys):
                source = lax.rem(y + ys - k, ys) * 2 + 1 - core
                wanted(source, h, lambda: arrived(source, t, h))

    def every(source, h, do):
        do()

    def piece(s, n, q):
        return xl.at[s, n, pl.ds(q * piece_rows, piece_rows)]

    def down(s, n, q):
        return pltpu.make_async_remote_copy(
            src_ref=piece(s, n, q),
            dst_ref=piece(s, n, q),
            send_sem=z_send.at[n, q],
            recv_sem=x_recv.at[s, n, q],
            device_id={"row": r + 2},
            device_id_type=MESH,
        )

    def across(s, n, q):
        return pltpu.make_async_remote_copy(
            src_ref=piece(s, n, q),
            dst_ref=piece(s, n, q),
            send_sem=x_send.at[n, q],
            recv_sem=x_recv.at[s, n, q],
            device_id={"row": depth * 2 + 1 - line},
            device_id_type=MESH,
        )

    def forward(n, q):
        across(line, n, q).start()

        @pl.when(depth < depths - 1)
        def _():
            down(line, n, q).start()

    def lanes(n):
        return pl.ds(pl.multiple_of(n * LANES, LANES), LANES)

    def product(s, t, n):
        total = None
        for j in range(half):
            term = mm(gat[s * half + j, t], xl[s, n, pl.ds(j * cw, cw)])
            total = term if total is None else total + term
        return total

    middle = width // 2

    def tile_part(below_by, first):
        for j in range(half):
            at = (first + below_by) * middle
            if j // (half // 2) == first:
                low_tri[at : at + middle, j * cw : (j + 1) * cw] = gat[
                    line * half + j, 0, at : at + middle
                ]

    def recip_of(first):
        ps = [piv[line * half + first * (half // 2) + j] for j in range(half // 2)]
        return 1.0 / (ps[0] if len(ps) == 1 else jnp.concatenate(ps, axis=1))

    def keep(at, to, value):
        high, low = split(value)
        inv_hi[at : at + middle, to : to + middle] = high
        inv_lo[at : at + middle, to : to + middle] = low

    def diagonal_halves():
        for d in range(1, cols):
            pivot_copy(d, lax.rem(c + d, cols)).wait_recv()
        piv[c] = pivots[...]
        row = lax.broadcasted_iota(jnp.int32, (middle, middle), 0)
        col = lax.broadcasted_iota(jnp.int32, (middle, middle), 1)
        parts = []
        for i in range(2):
            tile_part(0, i)
            at = i * middle
            recip = recip_of(i)
            here = low_tri[at : at + middle, at : at + middle].astype(F32)
            parts.append(jnp.where(row > col, here * recip, 0.0))
            scale[at : at + middle] = jnp.broadcast_to(
                jnp.sum(jnp.where(row == col, recip, 0.0), axis=1, keepdims=True),
                (middle, LANES),
            )
        for i, inverse in enumerate(unit_inverses(parts)):
            ends[i] = inverse
            keep(i * middle, i * middle, inverse)
        keep(0, middle, jnp.zeros((middle, middle), F32))

    def corner():
        tile_part(1, 0)
        here = low_tri[middle:, :middle].astype(F32) * recip_of(0)
        keep(middle, 0, -mm3(ends[1], mm3(here, ends[0])))

    @pl.when(r == 0)
    def _():
        take(0, lambda source, h, do: pl.when(below(source, h) == 0)(do))
        diagonal_halves()
        take(
            0,
            lambda source, h, do: pl.when((source < half) & (below(source, h) > 0))(do),
        )
        corner()

    @pl.when(r > 0)
    def _():
        take(0, every)

    @pl.when(r == 1)
    def _():
        diagonal_halves()
        corner()

    rhs_copy.wait()

    @pl.when(r == 0)
    def _():
        @pl.loop(0, chunks)
        def _(n):
            side = rhs[0, :, lanes(n)]
            x = (mm(inv_hi[...], side) + mm(inv_lo[...], side)) * scale[...]
            xl[0, n] = x.astype(BF16)
            out[0, :, lanes(n)] = x
            for q in range(PIECES):
                forward(n, q)

    @pl.when(r == 1)
    def _():
        @pl.loop(0, chunks)
        def _(n):
            for q in range(PIECES):
                across(0, n, q).wait_recv()
            side = rhs[0, :, lanes(n)].astype(F32) - product(0, 0, n)
            high, low = split(side)
            x = (mm(inv_hi[...], high) + mm(inv_lo[...], high) + mm(inv_hi[...], low)) * scale[...]
            xl[1, n] = x.astype(BF16)
            out[0, :, lanes(n)] = x
            for q in range(PIECES):
                forward(n, q)

    for t in range(1, layers):
        take(t, every)

    def leave(n):
        return pltpu.make_async_copy(
            out.at[:, :, lanes(n)], out_to.at[:, :, lanes(n)], out_sem.at[n]
        )

    def start(t, n):
        return rhs[t, :, lanes(n)].astype(F32)

    @pl.when(line == 0)
    def _():
        @pl.loop(0, chunks)
        def _(n):
            @pl.when(depth > 0)
            def _():
                for q in range(PIECES):
                    across(0, n, q).wait_recv()
                    forward(n, q)
                out[0, :, lanes(n)] = start(0, n) - product(0, 0, n)

            for t in range(1, layers):
                out[t, :, lanes(n)] = start(t, n) - product(0, t, n)

        @pl.loop(0, chunks)
        def _(n):
            for q in range(PIECES):
                across(1, n, q).wait_recv()

            @pl.when(depth > 0)
            def _():
                out[0, :, lanes(n)] -= product(1, 0, n)

            for t in range(1, layers):
                out[t, :, lanes(n)] -= product(1, t, n)
            leave(n).start()

    @pl.when(line == 1)
    def _():
        @pl.loop(0, chunks)
        def _(n):
            @pl.when(depth > 0)
            def _():
                for q in range(PIECES):
                    across(1, n, q).wait_recv()
                    forward(n, q)
                for q in range(PIECES):
                    across(0, n, q).wait_recv()
                out[0, :, lanes(n)] = start(0, n) - product(0, 0, n) - product(1, 0, n)

            for t in range(1, layers):
                out[t, :, lanes(n)] = start(t, n) - product(0, t, n) - product(1, t, n)
            leave(n).start()

    for t in range(layers):
        for h in range(HALVES):
            for k in range(ys):
                when_needed(c, t, h, lambda: own(k, t, h).wait_send())
            for k in range(1, ys):
                source = lax.rem(y + ys - k, ys) * 2 + core
                when_needed(source, t, h, lambda: relay(k, t, h).wait_send())

    @pl.when(depth == 0)
    def _():
        for d in range(1, cols):
            pivot_copy(d, c).wait_send()

    @pl.loop(0, chunks)
    def _(n):
        for q in range(PIECES):
            across(line, n, q).wait_send()

            @pl.when(depth < depths - 1)
            def _():
                down(line, n, q).wait_send()

        leave(n).wait()


def on_device(rows, cols, rhs, panel, pivots):
    layers, width, columns = rhs.shape
    cw = panel.shape[2]
    pw = pivots.shape[0]
    ys = cols // 2
    chunks = columns // LANES
    dma = pltpu.SemaphoreType.DMA
    vmem = pl.BlockSpec(memory_space=pltpu.VMEM)
    anywhere = pl.BlockSpec(memory_space=pl.ANY)
    far = pl.BlockSpec(memory_space=pltpu.HBM)
    return pl.pallas_call(
        functools.partial(kernel, rows, cols),
        out_shape=jax.ShapeDtypeStruct((layers, width, columns), F32),
        in_specs=[far, far, vmem],
        out_specs=anywhere,
        scratch_shapes=[
            pltpu.VMEM((layers, width, columns), BF16),
            pltpu.VMEM((layers, width, columns), F32),
            pltpu.VMEM((cols, layers, width, cw), BF16),
            pltpu.VMEM((cols, 1, pw), F32),
            pltpu.VMEM((2, chunks, width, LANES), BF16),
            pltpu.VMEM((width, width), BF16),
            pltpu.VMEM((width, width), BF16),
            pltpu.VMEM((width, width), BF16),
            pltpu.VMEM((width, LANES), F32),
            pltpu.VMEM((2, width // 2, width // 2), F32),
            dma((ys, layers, HALVES)),
            dma((cols, layers, HALVES)),
            dma((ys, layers, HALVES)),
            dma((cols,)),
            dma((cols,)),
            dma((chunks, PIECES)),
            dma((chunks, PIECES)),
            dma((2, chunks, PIECES)),
            dma((2,)),
            dma((chunks,)),
        ],
        compiler_params=pltpu.CompilerParams(
            collective_id=0, has_side_effects=True, vmem_limit_bytes=24 * 1024 * 1024
        ),
        name="solve_and_update",
    )(rhs, panel, pivots.reshape(1, pw))


def solution(mesh):
    placed = (P(None, "row", "col"), P(None, "row", "col"), P("col"))
    return jax.shard_map(
        functools.partial(on_device, mesh.shape["row"], mesh.shape["col"]),
        mesh=mesh,
        in_specs=placed,
        out_specs=P(None, "row", "col"),
        check_vma=False,
    )
```

```python
import functools

import jax
import jax.numpy as jnp
from jax import lax
from jax.experimental import pallas as pl
from jax.experimental.pallas import tpu as pltpu
from jax.sharding import PartitionSpec as P

MESH = pl.DeviceIdType.MESH
LANES = 128
PIECES = 4
HALVES = 4
F32 = jnp.float32
BF16 = jnp.bfloat16


def mm(a, b):
    return jnp.dot(a, b, preferred_element_type=F32)


def split(a):
    high = a.astype(BF16)
    return high, (a - high.astype(F32)).astype(BF16)


def mm3(a, b):
    ah, al = split(a)
    bh, bl = split(b)
    return mm(ah, bh) + (mm(ah, bl) + mm(al, bh))


def unit_inverses(parts):
    size, whole = LANES, parts[0].shape[0]
    row = lax.broadcasted_iota(jnp.int32, (LANES, LANES), 0)
    col = lax.broadcasted_iota(jnp.int32, (LANES, LANES), 1)
    base = 4
    blocks = [n[i : i + LANES, i : i + LANES] for n in parts for i in range(0, whole, LANES)]
    power = [jnp.where((row >> base) == (col >> base), b, 0.0) for b in blocks]
    done = [jnp.where(row == col, 1.0, 0.0) - p for p in power]
    for _ in range(base - 1):
        power = [mm3(p, p) for p in power]
        done = [d + mm3(d, p) for d, p in zip(done, power)]
    shift = base
    while (1 << shift) < LANES:
        inside = ((row >> (shift + 1)) == (col >> (shift + 1))) & (
            (row >> shift) != (col >> shift)
        )
        right = [mm3(jnp.where(inside, b, 0.0), d) for b, d in zip(blocks, done)]
        done = [d - mm3(d, m) for d, m in zip(done, right)]
        shift += 1
    while size < whole:
        each = whole // (2 * size)
        pairs = []
        for i in range(0, len(done), 2):
            n, at = parts[i // 2 // each], (i // 2 % each) * 2 * size
            top, low = done[i], done[i + 1]
            corner = -mm3(low, mm3(n[at + size : at + 2 * size, at : at + size], top))
            first = jnp.concatenate([top, jnp.zeros((size, size), F32)], axis=1)
            pairs.append(
                jnp.concatenate([first, jnp.concatenate([corner, low], axis=1)], axis=0)
            )
        done = pairs
        size *= 2
    return done


def kernel(
    rows,
    cols,
    rhs_in,
    panel_in,
    pivots,
    out_to,
    rhs,
    out,
    gat,
    piv,
    xl,
    low_tri,
    inv_hi,
    inv_lo,
    scale,
    ends,
    g_send,
    g_recv,
    f_send,
    p_send,
    p_recv,
    z_send,
    x_send,
    x_recv,
    in_sem,
    out_sem,
):
    r = lax.axis_index("row")
    c = lax.axis_index("col")
    line = lax.rem(r, 2)
    depth = r // 2
    depths = rows // 2
    hub = depths // 2
    onward = (depth == 0) | ((depth >= hub) & (depth < depths - 1))
    backward = (depth >= 2) & (depth <= hub)
    layers, width, columns = rhs.shape
    cw = panel_in.shape[2]
    half = cols // 2
    ys = cols // 2
    y, core = c // 2, lax.rem(c, 2)
    chunks = columns // LANES
    piece_rows = width // PIECES
    part_rows = width // HALVES
    partner = y * 2 + 1 - core

    panel_copy = pltpu.make_async_copy(panel_in, gat.at[c], in_sem.at[0])
    rhs_copy = pltpu.make_async_copy(rhs_in, rhs, in_sem.at[1])
    panel_copy.start()
    rhs_copy.start()

    barrier = pltpu.get_barrier_semaphore()
    for d in range(1, cols):
        pl.semaphore_signal(
            barrier, inc=1, device_id={"col": lax.rem(c + d, cols)}, device_id_type=MESH
        )
    pl.semaphore_signal(
        barrier, inc=1, device_id={"row": depth * 2 + 1 - line}, device_id_type=MESH
    )

    meets = [
        (depth == 0, hub),
        (depth == hub, 0),
        (depth >= 2, depth - 1),
        ((depth >= 1) & (depth < depths - 1), depth + 1),
    ]
    peers = cols
    for there, other_depth in meets:

        @pl.when(there)
        def _():
            pl.semaphore_signal(
                barrier,
                inc=1,
                device_id={"row": other_depth * 2 + line},
                device_id_type=MESH,
            )

        peers = peers + jnp.where(there, 1, 0)
    pl.semaphore_wait(barrier, peers)

    def own(k, t, h):
        part = pl.ds(h * part_rows, part_rows)
        target = partner if k == 0 else lax.rem(y + k, ys) * 2 + core
        return pltpu.make_async_remote_copy(
            src_ref=gat.at[c, t, part],
            dst_ref=gat.at[c, t, part],
            send_sem=g_send.at[k, t, h],
            recv_sem=g_recv.at[c, t, h],
            device_id={"col": target},
            device_id_type=MESH,
        )

    def relay(k, t, h):
        part = pl.ds(h * part_rows, part_rows)
        source = lax.rem(y + ys - k, ys) * 2 + core
        return pltpu.make_async_remote_copy(
            src_ref=gat.at[source, t, part],
            dst_ref=gat.at[source, t, part],
            send_sem=f_send.at[k, t, h],
            recv_sem=g_recv.at[source, t, h],
            device_id={"col": partner},
            device_id_type=MESH,
        )

    def arrived(source, t, h):
        part = pl.ds(h * part_rows, part_rows)
        pltpu.make_async_remote_copy(
            src_ref=gat.at[source, t, part],
            dst_ref=gat.at[source, t, part],
            send_sem=f_send.at[0, t, h],
            recv_sem=g_recv.at[source, t, h],
            device_id={"col": partner},
            device_id_type=MESH,
        ).wait_recv()

    def pivot_copy(d, source):
        return pltpu.make_async_remote_copy(
            src_ref=pivots,
            dst_ref=piv.at[source],
            send_sem=p_send.at[d],
            recv_sem=p_recv.at[source],
            device_id={"col": lax.rem(c + d, cols)},
            device_id_type=MESH,
        )

    @pl.when(depth == 0)
    def _():
        for d in range(1, cols):
            pivot_copy(d, c).start()

    def below(source, h):
        return h // (HALVES // 2) - source // (half // 2)

    def when_needed(source, t, h, do):
        if t > 0:
            do()
        else:
            pl.when((r > 0) | (below(source, h) >= 0))(do)

    panel_copy.wait()
    for t in range(layers):
        for h in range(HALVES):
            for k in range(ys - 1, -1, -1):
                when_needed(c, t, h, lambda: own(k, t, h).start())

    def take(t, wanted):
        for h in range(HALVES):
            for k in range(1, ys):
                source = lax.rem(y + ys - k, ys) * 2 + core

                def pass_on():
                    arrived(source, t, h)
                    relay(k, t, h).start()

                wanted(source, h, pass_on)
        for h in range(HALVES):
            for k in range(ys):
                source = lax.rem(y + ys - k, ys) * 2 + 1 - core
                wanted(source, h, lambda: arrived(source, t, h))

    def every(source, h, do):
        do()

    def piece(s, n, q):
        return xl.at[s, n, pl.ds(q * piece_rows, piece_rows)]

    def down(way, s, n, q):
        target = depth - 1 if way else jnp.where(depth == 0, hub, depth + 1)
        return pltpu.make_async_remote_copy(
            src_ref=piece(s, n, q),
            dst_ref=piece(s, n, q),
            send_sem=z_send.at[way, n, q],
            recv_sem=x_recv.at[s, n, q],
            device_id={"row": target * 2 + line},
            device_id_type=MESH,
        )

    def across(s, n, q):
        return pltpu.make_async_remote_copy(
            src_ref=piece(s, n, q),
            dst_ref=piece(s, n, q),
            send_sem=x_send.at[n, q],
            recv_sem=x_recv.at[s, n, q],
            device_id={"row": depth * 2 + 1 - line},
            device_id_type=MESH,
        )

    def forward(n, q):
        for way, there in enumerate((onward, backward)):

            @pl.when(there)
            def _():
                down(way, line, n, q).start()

        across(line, n, q).start()

    def lanes(n):
        return pl.ds(pl.multiple_of(n * LANES, LANES), LANES)

    def product(s, t, n):
        total = None
        for j in range(half):
            term = mm(gat[s * half + j, t], xl[s, n, pl.ds(j * cw, cw)])
            total = term if total is None else total + term
        return total

    middle = width // 2

    def tile_part(below_by, first):
        for j in range(half):
            at = (first + below_by) * middle
            if j // (half // 2) == first:
                low_tri[at : at + middle, j * cw : (j + 1) * cw] = gat[
                    line * half + j, 0, at : at + middle
                ]

    def recip_of(first):
        ps = [piv[line * half + first * (half // 2) + j] for j in range(half // 2)]
        return 1.0 / (ps[0] if len(ps) == 1 else jnp.concatenate(ps, axis=1))

    def keep(at, to, value):
        high, low = split(value)
        inv_hi[at : at + middle, to : to + middle] = high
        inv_lo[at : at + middle, to : to + middle] = low

    def diagonal_halves():
        for d in range(1, cols):
            pivot_copy(d, lax.rem(c + d, cols)).wait_recv()
        piv[c] = pivots[...]
        row = lax.broadcasted_iota(jnp.int32, (middle, middle), 0)
        col = lax.broadcasted_iota(jnp.int32, (middle, middle), 1)
        parts = []
        for i in range(2):
            tile_part(0, i)
            at = i * middle
            recip = recip_of(i)
            here = low_tri[at : at + middle, at : at + middle].astype(F32)
            parts.append(jnp.where(row > col, here * recip, 0.0))
            scale[at : at + middle] = jnp.broadcast_to(
                jnp.sum(jnp.where(row == col, recip, 0.0), axis=1, keepdims=True),
                (middle, LANES),
            )
        for i, inverse in enumerate(unit_inverses(parts)):
            ends[i] = inverse
            keep(i * middle, i * middle, inverse)
        keep(0, middle, jnp.zeros((middle, middle), F32))

    def corner():
        tile_part(1, 0)
        here = low_tri[middle:, :middle].astype(F32) * recip_of(0)
        keep(middle, 0, -mm3(ends[1], mm3(here, ends[0])))

    @pl.when(r == 0)
    def _():
        take(0, lambda source, h, do: pl.when(below(source, h) == 0)(do))
        diagonal_halves()
        take(
            0,
            lambda source, h, do: pl.when((source < half) & (below(source, h) > 0))(do),
        )
        corner()

    @pl.when(r > 0)
    def _():
        take(0, every)

    @pl.when(r == 1)
    def _():
        diagonal_halves()
        corner()

    rhs_copy.wait()

    @pl.when(r == 0)
    def _():
        @pl.loop(0, chunks)
        def _(n):
            side = rhs[0, :, lanes(n)]
            x = (mm(inv_hi[...], side) + mm(inv_lo[...], side)) * scale[...]
            xl[0, n] = x.astype(BF16)
            out[0, :, lanes(n)] = x
            for q in range(PIECES):
                forward(n, q)

    @pl.when(r == 1)
    def _():
        @pl.loop(0, chunks)
        def _(n):
            for q in range(PIECES):
                across(0, n, q).wait_recv()
            side = rhs[0, :, lanes(n)].astype(F32) - product(0, 0, n)
            high, low = split(side)
            x = (mm(inv_hi[...], high) + mm(inv_lo[...], high) + mm(inv_hi[...], low)) * scale[...]
            xl[1, n] = x.astype(BF16)
            out[0, :, lanes(n)] = x
            for q in range(PIECES):
                forward(n, q)

    for t in range(1, layers):
        take(t, every)

    def leave(n):
        return pltpu.make_async_copy(
            out.at[:, :, lanes(n)], out_to.at[:, :, lanes(n)], out_sem.at[n]
        )

    def start(t, n):
        return rhs[t, :, lanes(n)].astype(F32)

    @pl.when(line == 0)
    def _():
        @pl.loop(0, chunks)
        def _(n):
            @pl.when(depth > 0)
            def _():
                for q in range(PIECES):
                    across(0, n, q).wait_recv()
                    forward(n, q)
                out[0, :, lanes(n)] = start(0, n) - product(0, 0, n)

            for t in range(1, layers):
                out[t, :, lanes(n)] = start(t, n) - product(0, t, n)

        @pl.loop(0, chunks)
        def _(n):
            for q in range(PIECES):
                across(1, n, q).wait_recv()

            @pl.when(depth > 0)
            def _():
                out[0, :, lanes(n)] -= product(1, 0, n)

            for t in range(1, layers):
                out[t, :, lanes(n)] -= product(1, t, n)
            leave(n).start()

    @pl.when(line == 1)
    def _():
        @pl.loop(0, chunks)
        def _(n):
            @pl.when(depth > 0)
            def _():
                for q in range(PIECES):
                    across(1, n, q).wait_recv()
                    forward(n, q)
                for q in range(PIECES):
                    across(0, n, q).wait_recv()
                out[0, :, lanes(n)] = start(0, n) - product(0, 0, n) - product(1, 0, n)

            for t in range(1, layers):
                out[t, :, lanes(n)] = start(t, n) - product(0, t, n) - product(1, t, n)
            leave(n).start()

    for t in range(layers):
        for h in range(HALVES):
            for k in range(ys):
                when_needed(c, t, h, lambda: own(k, t, h).wait_send())
            for k in range(1, ys):
                source = lax.rem(y + ys - k, ys) * 2 + core
                when_needed(source, t, h, lambda: relay(k, t, h).wait_send())

    @pl.when(depth == 0)
    def _():
        for d in range(1, cols):
            pivot_copy(d, c).wait_send()

    @pl.loop(0, chunks)
    def _(n):
        for q in range(PIECES):
            across(line, n, q).wait_send()

            for way, there in enumerate((onward, backward)):

                @pl.when(there)
                def _():
                    down(way, line, n, q).wait_send()

        leave(n).wait()


def on_device(rows, cols, rhs, panel, pivots):
    layers, width, columns = rhs.shape
    cw = panel.shape[2]
    pw = pivots.shape[0]
    ys = cols // 2
    chunks = columns // LANES
    dma = pltpu.SemaphoreType.DMA
    vmem = pl.BlockSpec(memory_space=pltpu.VMEM)
    anywhere = pl.BlockSpec(memory_space=pl.ANY)
    far = pl.BlockSpec(memory_space=pltpu.HBM)
    return pl.pallas_call(
        functools.partial(kernel, rows, cols),
        out_shape=jax.ShapeDtypeStruct((layers, width, columns), F32),
        in_specs=[far, far, vmem],
        out_specs=anywhere,
        scratch_shapes=[
            pltpu.VMEM((layers, width, columns), BF16),
            pltpu.VMEM((layers, width, columns), F32),
            pltpu.VMEM((cols, layers, width, cw), BF16),
            pltpu.VMEM((cols, 1, pw), F32),
            pltpu.VMEM((2, chunks, width, LANES), BF16),
            pltpu.VMEM((width, width), BF16),
            pltpu.VMEM((width, width), BF16),
            pltpu.VMEM((width, width), BF16),
            pltpu.VMEM((width, LANES), F32),
            pltpu.VMEM((2, width // 2, width // 2), F32),
            dma((ys, layers, HALVES)),
            dma((cols, layers, HALVES)),
            dma((ys, layers, HALVES)),
            dma((cols,)),
            dma((cols,)),
            dma((2, chunks, PIECES)),
            dma((chunks, PIECES)),
            dma((2, chunks, PIECES)),
            dma((2,)),
            dma((chunks,)),
        ],
        compiler_params=pltpu.CompilerParams(
            collective_id=0, has_side_effects=True, vmem_limit_bytes=24 * 1024 * 1024
        ),
        name="solve_and_update",
    )(rhs, panel, pivots.reshape(1, pw))


def solution(mesh):
    placed = (P(None, "row", "col"), P(None, "row", "col"), P("col"))
    return jax.shard_map(
        functools.partial(on_device, mesh.shape["row"], mesh.shape["col"]),
        mesh=mesh,
        in_specs=placed,
        out_specs=P(None, "row", "col"),
        check_vma=False,
    )
```

```python
import functools

import jax
import jax.numpy as jnp
from jax import lax
from jax.experimental import pallas as pl
from jax.experimental.pallas import tpu as pltpu
from jax.sharding import PartitionSpec as P

MESH = pl.DeviceIdType.MESH
LANES = 128
PIECES = 4
HALVES = 4
F32 = jnp.float32
BF16 = jnp.bfloat16


def mm(a, b):
    return jnp.dot(a, b, preferred_element_type=F32)


def split(a):
    high = a.astype(BF16)
    return high, (a - high.astype(F32)).astype(BF16)


def mm3(a, b):
    ah, al = split(a)
    bh, bl = split(b)
    return mm(ah, bh) + (mm(ah, bl) + mm(al, bh))


def unit_inverses(parts):
    size, whole = LANES, parts[0].shape[0]
    row = lax.broadcasted_iota(jnp.int32, (LANES, LANES), 0)
    col = lax.broadcasted_iota(jnp.int32, (LANES, LANES), 1)
    base = 4
    blocks = [n[i : i + LANES, i : i + LANES] for n in parts for i in range(0, whole, LANES)]
    power = [jnp.where((row >> base) == (col >> base), b, 0.0) for b in blocks]
    done = [jnp.where(row == col, 1.0, 0.0) - p for p in power]
    for _ in range(base - 1):
        power = [mm3(p, p) for p in power]
        done = [d + mm3(d, p) for d, p in zip(done, power)]
    shift = base
    while (1 << shift) < LANES:
        inside = ((row >> (shift + 1)) == (col >> (shift + 1))) & (
            (row >> shift) != (col >> shift)
        )
        right = [mm3(jnp.where(inside, b, 0.0), d) for b, d in zip(blocks, done)]
        done = [d - mm3(d, m) for d, m in zip(done, right)]
        shift += 1
    while size < whole:
        each = whole // (2 * size)
        pairs = []
        for i in range(0, len(done), 2):
            n, at = parts[i // 2 // each], (i // 2 % each) * 2 * size
            top, low = done[i], done[i + 1]
            corner = -mm3(low, mm3(n[at + size : at + 2 * size, at : at + size], top))
            first = jnp.concatenate([top, jnp.zeros((size, size), F32)], axis=1)
            pairs.append(
                jnp.concatenate([first, jnp.concatenate([corner, low], axis=1)], axis=0)
            )
        done = pairs
        size *= 2
    return done


def kernel(
    rows,
    cols,
    rhs_in,
    panel_in,
    pivots,
    out_to,
    rhs,
    out,
    gat,
    piv,
    xl,
    low_tri,
    inv_hi,
    inv_lo,
    scale,
    ends,
    g_send,
    g_recv,
    f_send,
    p_send,
    p_recv,
    z_send,
    x_send,
    x_recv,
    in_sem,
    out_sem,
):
    r = lax.axis_index("row")
    c = lax.axis_index("col")
    line = lax.rem(r, 2)
    depth = r // 2
    depths = rows // 2
    hub = depths // 2
    onward = (depth == 0) | ((depth >= hub) & (depth < depths - 1))
    backward = (depth >= 2) & (depth <= hub)
    layers, width, columns = rhs.shape
    cw = panel_in.shape[2]
    half = cols // 2
    ys = cols // 2
    y, core = c // 2, lax.rem(c, 2)
    chunks = columns // LANES
    piece_rows = width // PIECES
    part_rows = width // HALVES
    partner = y * 2 + 1 - core

    panel_copy = pltpu.make_async_copy(panel_in, gat.at[c], in_sem.at[0])
    rhs_copy = pltpu.make_async_copy(rhs_in, rhs, in_sem.at[1])
    panel_copy.start()
    rhs_copy.start()

    barrier = pltpu.get_barrier_semaphore()
    for d in range(1, cols):
        pl.semaphore_signal(
            barrier, inc=1, device_id={"col": lax.rem(c + d, cols)}, device_id_type=MESH
        )
    pl.semaphore_signal(
        barrier, inc=1, device_id={"row": depth * 2 + 1 - line}, device_id_type=MESH
    )

    meets = [
        (depth == 0, hub),
        (depth == hub, 0),
        (depth >= 2, depth - 1),
        ((depth >= 1) & (depth < depths - 1), depth + 1),
    ]
    peers = cols
    for there, other_depth in meets:

        @pl.when(there)
        def _():
            pl.semaphore_signal(
                barrier,
                inc=1,
                device_id={"row": other_depth * 2 + line},
                device_id_type=MESH,
            )

        peers = peers + jnp.where(there, 1, 0)
    pl.semaphore_wait(barrier, peers)

    def own(k, t, h):
        part = pl.ds(h * part_rows, part_rows)
        target = partner if k == 0 else lax.rem(y + k, ys) * 2 + core
        return pltpu.make_async_remote_copy(
            src_ref=gat.at[c, t, part],
            dst_ref=gat.at[c, t, part],
            send_sem=g_send.at[k, t, h],
            recv_sem=g_recv.at[c, t, h],
            device_id={"col": target},
            device_id_type=MESH,
        )

    def relay(k, t, h):
        part = pl.ds(h * part_rows, part_rows)
        source = lax.rem(y + ys - k, ys) * 2 + core
        return pltpu.make_async_remote_copy(
            src_ref=gat.at[source, t, part],
            dst_ref=gat.at[source, t, part],
            send_sem=f_send.at[k, t, h],
            recv_sem=g_recv.at[source, t, h],
            device_id={"col": partner},
            device_id_type=MESH,
        )

    def arrived(source, t, h):
        part = pl.ds(h * part_rows, part_rows)
        pltpu.make_async_remote_copy(
            src_ref=gat.at[source, t, part],
            dst_ref=gat.at[source, t, part],
            send_sem=f_send.at[0, t, h],
            recv_sem=g_recv.at[source, t, h],
            device_id={"col": partner},
            device_id_type=MESH,
        ).wait_recv()

    def pivot_copy(d, source):
        return pltpu.make_async_remote_copy(
            src_ref=pivots,
            dst_ref=piv.at[source],
            send_sem=p_send.at[d],
            recv_sem=p_recv.at[source],
            device_id={"col": lax.rem(c + d, cols)},
            device_id_type=MESH,
        )

    @pl.when(depth == 0)
    def _():
        for d in range(1, cols):
            pivot_copy(d, c).start()

    def below(source, h):
        return h // (HALVES // 2) - source // (half // 2)

    def when_needed(source, t, h, do):
        if t > 0:
            do()
        else:
            pl.when((r > 0) | (below(source, h) >= 0))(do)

    panel_copy.wait()
    for t in range(layers):
        for h in range(HALVES):
            for k in range(ys - 1, -1, -1):
                when_needed(c, t, h, lambda: own(k, t, h).start())

    def take(t, wanted):
        for h in range(HALVES):
            for k in range(1, ys):
                source = lax.rem(y + ys - k, ys) * 2 + core

                def pass_on():
                    arrived(source, t, h)
                    relay(k, t, h).start()

                wanted(source, h, pass_on)
        for h in range(HALVES):
            for k in range(ys):
                source = lax.rem(y + ys - k, ys) * 2 + 1 - core
                wanted(source, h, lambda: arrived(source, t, h))

    def every(source, h, do):
        do()

    def piece(s, n, q):
        return xl.at[s, n, pl.ds(q * piece_rows, piece_rows)]

    def down(way, s, n, q):
        target = depth - 1 if way else jnp.where(depth == 0, hub, depth + 1)
        return pltpu.make_async_remote_copy(
            src_ref=piece(s, n, q),
            dst_ref=piece(s, n, q),
            send_sem=z_send.at[way, n, q],
            recv_sem=x_recv.at[s, n, q],
            device_id={"row": target * 2 + line},
            device_id_type=MESH,
        )

    def across(s, n, q):
        return pltpu.make_async_remote_copy(
            src_ref=piece(s, n, q),
            dst_ref=piece(s, n, q),
            send_sem=x_send.at[n, q],
            recv_sem=x_recv.at[s, n, q],
            device_id={"row": depth * 2 + 1 - line},
            device_id_type=MESH,
        )

    def forward(n, q):
        for way, there in enumerate((onward, backward)):

            @pl.when(there)
            def _():
                down(way, line, n, q).start()

        across(line, n, q).start()

    def lanes(n):
        return pl.ds(pl.multiple_of(n * LANES, LANES), LANES)

    def product(s, t, n):
        total = None
        for j in range(half):
            term = mm(gat[s * half + j, t], xl[s, n, pl.ds(j * cw, cw)])
            total = term if total is None else total + term
        return total

    middle = width // 2

    def tile_part(below_by, first):
        for j in range(half):
            at = (first + below_by) * middle
            if j // (half // 2) == first:
                low_tri[at : at + middle, j * cw : (j + 1) * cw] = gat[
                    line * half + j, 0, at : at + middle
                ]

    def recip_of(first):
        ps = [piv[line * half + first * (half // 2) + j] for j in range(half // 2)]
        return 1.0 / (ps[0] if len(ps) == 1 else jnp.concatenate(ps, axis=1))

    def keep(at, to, value):
        high, low = split(value)
        inv_hi[at : at + middle, to : to + middle] = high
        inv_lo[at : at + middle, to : to + middle] = low

    def diagonal_halves():
        for d in range(1, cols):
            pivot_copy(d, lax.rem(c + d, cols)).wait_recv()
        piv[c] = pivots[...]
        row = lax.broadcasted_iota(jnp.int32, (middle, middle), 0)
        col = lax.broadcasted_iota(jnp.int32, (middle, middle), 1)
        parts = []
        for i in range(2):
            tile_part(0, i)
            at = i * middle
            recip = recip_of(i)
            here = low_tri[at : at + middle, at : at + middle].astype(F32)
            parts.append(jnp.where(row > col, here * recip, 0.0))
            scale[at : at + middle] = jnp.broadcast_to(
                jnp.sum(jnp.where(row == col, recip, 0.0), axis=1, keepdims=True),
                (middle, LANES),
            )
        for i, inverse in enumerate(unit_inverses(parts)):
            ends[i] = inverse
            keep(i * middle, i * middle, inverse)
        keep(0, middle, jnp.zeros((middle, middle), F32))

    def corner():
        tile_part(1, 0)
        here = low_tri[middle:, :middle].astype(F32) * recip_of(0)
        keep(middle, 0, -mm3(ends[1], mm3(here, ends[0])))

    @pl.when(r == 0)
    def _():
        take(0, lambda source, h, do: pl.when(below(source, h) == 0)(do))
        diagonal_halves()
        take(
            0,
            lambda source, h, do: pl.when((source < half) & (below(source, h) > 0))(do),
        )
        corner()

    @pl.when(r > 0)
    def _():
        take(0, every)

    @pl.when(r == 1)
    def _():
        diagonal_halves()
        corner()

    rhs_copy.wait()

    @pl.when(r == 0)
    def _():
        @pl.loop(0, chunks)
        def _(n):
            side = rhs[0, :, lanes(n)]
            x = (mm(inv_hi[...], side) + mm(inv_lo[...], side)) * scale[...]
            xl[0, n] = x.astype(BF16)
            out[0, :, lanes(n)] = x
            for q in range(PIECES):
                forward(n, q)

    @pl.when(r == 1)
    def _():
        @pl.loop(0, chunks)
        def _(n):
            for q in range(PIECES):
                across(0, n, q).wait_recv()
            side = rhs[0, :, lanes(n)].astype(F32) - product(0, 0, n)
            high, low = split(side)
            x = (mm(inv_hi[...], high) + mm(inv_lo[...], high) + mm(inv_hi[...], low)) * scale[...]
            xl[1, n] = x.astype(BF16)
            out[0, :, lanes(n)] = x
            for q in range(PIECES):
                forward(n, q)

    early = chunks // 2

    @pl.when(depth > 0)
    def _():
        @pl.loop(0, early)
        def _(n):
            for q in range(PIECES):
                across(line, n, q).wait_recv()
                forward(n, q)

    for t in range(1, layers):
        take(t, every)

    def leave(n):
        return pltpu.make_async_copy(
            out.at[:, :, lanes(n)], out_to.at[:, :, lanes(n)], out_sem.at[n]
        )

    def start(t, n):
        return rhs[t, :, lanes(n)].astype(F32)

    @pl.when(line == 0)
    def _():
        @pl.loop(0, chunks)
        def _(n):
            @pl.when(depth > 0)
            def _():
                @pl.when(n >= early)
                def _():
                    for q in range(PIECES):
                        across(0, n, q).wait_recv()
                        forward(n, q)

                out[0, :, lanes(n)] = start(0, n) - product(0, 0, n)

            for t in range(1, layers):
                out[t, :, lanes(n)] = start(t, n) - product(0, t, n)

        @pl.loop(0, chunks)
        def _(n):
            for q in range(PIECES):
                across(1, n, q).wait_recv()

            @pl.when(depth > 0)
            def _():
                out[0, :, lanes(n)] -= product(1, 0, n)

            for t in range(1, layers):
                out[t, :, lanes(n)] -= product(1, t, n)
            leave(n).start()

    @pl.when(line == 1)
    def _():
        @pl.loop(0, chunks)
        def _(n):
            @pl.when(depth > 0)
            def _():
                @pl.when(n >= early)
                def _():
                    for q in range(PIECES):
                        across(1, n, q).wait_recv()
                        forward(n, q)

                for q in range(PIECES):
                    across(0, n, q).wait_recv()
                out[0, :, lanes(n)] = start(0, n) - product(0, 0, n) - product(1, 0, n)

            for t in range(1, layers):
                out[t, :, lanes(n)] = start(t, n) - product(0, t, n) - product(1, t, n)
            leave(n).start()

    for t in range(layers):
        for h in range(HALVES):
            for k in range(ys):
                when_needed(c, t, h, lambda: own(k, t, h).wait_send())
            for k in range(1, ys):
                source = lax.rem(y + ys - k, ys) * 2 + core
                when_needed(source, t, h, lambda: relay(k, t, h).wait_send())

    @pl.when(depth == 0)
    def _():
        for d in range(1, cols):
            pivot_copy(d, c).wait_send()

    @pl.loop(0, chunks)
    def _(n):
        for q in range(PIECES):
            across(line, n, q).wait_send()

            for way, there in enumerate((onward, backward)):

                @pl.when(there)
                def _():
                    down(way, line, n, q).wait_send()

        leave(n).wait()


def on_device(rows, cols, rhs, panel, pivots):
    layers, width, columns = rhs.shape
    cw = panel.shape[2]
    pw = pivots.shape[0]
    ys = cols // 2
    chunks = columns // LANES
    dma = pltpu.SemaphoreType.DMA
    vmem = pl.BlockSpec(memory_space=pltpu.VMEM)
    anywhere = pl.BlockSpec(memory_space=pl.ANY)
    far = pl.BlockSpec(memory_space=pltpu.HBM)
    return pl.pallas_call(
        functools.partial(kernel, rows, cols),
        out_shape=jax.ShapeDtypeStruct((layers, width, columns), F32),
        in_specs=[far, far, vmem],
        out_specs=anywhere,
        scratch_shapes=[
            pltpu.VMEM((layers, width, columns), BF16),
            pltpu.VMEM((layers, width, columns), F32),
            pltpu.VMEM((cols, layers, width, cw), BF16),
            pltpu.VMEM((cols, 1, pw), F32),
            pltpu.VMEM((2, chunks, width, LANES), BF16),
            pltpu.VMEM((width, width), BF16),
            pltpu.VMEM((width, width), BF16),
            pltpu.VMEM((width, width), BF16),
            pltpu.VMEM((width, LANES), F32),
            pltpu.VMEM((2, width // 2, width // 2), F32),
            dma((ys, layers, HALVES)),
            dma((cols, layers, HALVES)),
            dma((ys, layers, HALVES)),
            dma((cols,)),
            dma((cols,)),
            dma((2, chunks, PIECES)),
            dma((chunks, PIECES)),
            dma((2, chunks, PIECES)),
            dma((2,)),
            dma((chunks,)),
        ],
        compiler_params=pltpu.CompilerParams(
            collective_id=0, has_side_effects=True, vmem_limit_bytes=24 * 1024 * 1024
        ),
        name="solve_and_update",
    )(rhs, panel, pivots.reshape(1, pw))


def solution(mesh):
    placed = (P(None, "row", "col"), P(None, "row", "col"), P("col"))
    return jax.shard_map(
        functools.partial(on_device, mesh.shape["row"], mesh.shape["col"]),
        mesh=mesh,
        in_specs=placed,
        out_specs=P(None, "row", "col"),
        check_vma=False,
    )
```
